256 devices in a mesh: row: 8 (over x, core), col: 8 (over z), fit: 4 (over y).
Axes of the slice: x: 4, y: 4, z: 8, core: 2. Of those that a mesh axis runs over, the one named last changes fastest.
Arguments:
- orbital_ints: bfloat16 [128, 40, 2560], P(('row', 'col'), None, 'fit'), may hold values from -0.83984375 to 0.83984375
- occ_energy: float32 [128], P(('row', 'col')), may hold values from -1.2 to -0.3
- pair_row: int32 [8192], P(('row', 'col')), may hold values from 0 to 15
- pair_col: int32 [8192], P(('row', 'col')), may hold values from 0 to 15
- virt_energy: float32 [40, 8192], P(None, ('row', 'col')), may hold values from 0.5 to 3
- amplitudes: float32 [40, 40, 8192], P(None, None, ('row', 'col')), may hold values from -1.8 to 1.8
- intersections: bfloat16 [40, 40, 16, 8192], P(None, None, 'fit', ('row', 'col')), may hold values from -1 to 1
- coupling_fock: float32 [16, 8192], P('fit', ('row', 'col')), may hold values from -0.25 to 0.25
- partner_owner: int32 [4, 8192, 4], P('fit', ('row', 'col')), may hold values from 0 to 63, all different within a row; in each aligned block of 128 rows (0 to 127, 128 to 255, ..., all dimensions but the last counted through in order) at most 16 rows name the same one
- partner_slot: int32 [4, 8192, 4], P('fit', ('row', 'col')), may hold values from 0 to 127
Outputs:
- new_amplitudes: float32 [40, 40, 8192], P(None, None, ('row', 'col'))
- residual: float32 [40, 40, 8192], P(None, None, ('row', 'col'))
The draws below stay inside these ranges and needn't reach their ends.
Inputs may be any that keep to these rules, and one draw needn't show every extreme that they name: `partner_owner`: the 4 owners of one pair in one fit index differ; among the pairs of one group in one fit index (aligned blocks of 128 rows) no owner is named more than 16 times, a bound that some block reaches.
All inputs are finite; a program needn't handle non-finite values.
Results may differ from the reference program's by a relative error of at most 0.014.
Values may be sent and summed in bfloat16 or wider, within the bound.
No kernel may reach another device: no remote copies, remote signals or barrier semaphores. Data moves between devices by JAX's collectives and lax.ppermute only.
A program may use at most 128 MiB of HBM per device.

```python
import math
import jax
import jax.numpy as jnp
import numpy as np
from jax import lax

NPNO = 40
NAUX = 2560
OCC_BLK = 2
PAIRS_DEV = 128
CPL_FIT = 4
ITERS = 2
OCC = 128
PAIRS = 8192
NCPL = 16
CAP = 16
N_ROW = 8
N_COL = 8
N_FIT = 4


def touch_ends(result, stream_key, low, largest):
    shape = result.shape
    spot = [jax.random.randint(jax.random.fold_in(stream_key, axis), (), 0, shape[axis]) for axis in range(len(shape))]
    result = result.at[tuple(spot)].set(low)
    longest = shape.index(max(shape))
    spot[longest] = (spot[longest] + 1) % shape[longest]
    return result.at[tuple(spot)].set(largest)


def level_of(own_key, shape, pieces, least, largest):
    factor_of, own = 1.0, jax.random.fold_in(own_key, 6)
    for position, parts in pieces:
        steps = jnp.exp(jax.random.uniform(jax.random.fold_in(own, position), (parts,), jnp.float32, least / len(pieces), largest / len(pieces)))
        factor_of = factor_of * jnp.repeat(steps, shape[position] // parts).reshape([-1 if axis == position else 1 for axis in range(len(shape))])
    return factor_of


def shared_out(own_key, own, number, rows, amount, top, most, slope):
    ranking = jax.random.permutation(own_key, amount)
    heavy_load, common = load_shares(amount, rows * top, most, slope, True), load_shares(amount, rows * top, most, slope, False)
    places = jnp.arange(amount)

    def named(tallies, rotation):
        used = int((tallies > 0).sum())
        fixed = max(1, used // 4)
        shifted = fixed + (places - fixed + rotation * (used - fixed)) % max(1, amount - fixed)
        return jnp.zeros((amount,), jnp.int32).at[ranking[jnp.where(places < fixed, places, shifted)]].set(jnp.asarray(tallies, jnp.int32))

    tallies = jnp.where(number % 4 == 0, named(heavy_load, number // 4), named(common, number - number // 4 - 1))
    mixed = jax.random.permutation(jax.random.fold_in(own, 3), amount)
    giver, receiver = mixed[0:amount // 2 * 2:2], mixed[1:amount // 2 * 2:2]
    margin = jnp.minimum(tallies[giver] - 1, most - tallies[receiver]) // 2
    margin = jnp.where((giver == ranking[0]) | (receiver == ranking[0]) | (tallies[receiver] == 0), 0, jnp.maximum(margin, 0))
    shifted = jax.random.randint(jax.random.fold_in(own, 4), (amount // 2,), 0, 1 << 20) % (margin + 1)
    tallies = tallies.at[giver].add(-shifted).at[receiver].add(shifted)
    items = jnp.searchsorted(jnp.cumsum(tallies), jnp.arange(rows * top), side="right").astype(jnp.int32)
    listing = items.reshape(top, rows).T
    listing = listing[jax.random.permutation(jax.random.fold_in(own, 1), rows)]
    rotation = jax.random.randint(jax.random.fold_in(own, 2), (rows, 1), 0, top)
    return jnp.take_along_axis(listing, (jnp.arange(top)[None, :] + rotation) % top, axis=1)


def load_shares(count, total, most, skew, full):
    portions = [(1 << 20) // math.isqrt(rank ** skew) + 1 for rank in range(1, count + 1)]
    largest = most if full else min(most, max(-(-total // count), total * portions[0] // sum(portions)))
    least = 1 if total - largest >= count - 1 else 0
    holding, surplus = [largest] + [least] * (count - 1), total - largest - least * (count - 1)
    while surplus > 0:
        free = [i for i in range(1, count) if holding[i] < largest] or [i for i in range(1, count) if holding[i] < most]
        pool, budget = sum([portions[i] for i in free]), surplus
        for i in free:
            addition = min(most - holding[i], max(1, budget * portions[i] // pool), surplus)
            holding[i] = holding[i] + addition
            surplus = surplus - addition
    return np.array(holding)


def centred(rng, extent, spread, limit, split=(), kind=jnp.bfloat16):
    values = jax.random.normal(rng, extent, jnp.float32) * spread
    if len(split) > 0:
        values = level_of(rng, extent, split, -0.22, 0.18) * values
    return jnp.clip(values, min=-limit, max=limit).astype(kind)


def setup_inputs(seed: int = 0) -> dict:
    streams_of = jax.random.split(jax.random.key(seed), 11)
    orbital_ints = centred(streams_of[0], (OCC, NPNO, NAUX), 0.14, 0.83984375, ((0, 64), (2, 4)))
    occ_energy = jnp.clip(-1.2 + 0.90000004 * jax.random.uniform(streams_of[1], (OCC,), jnp.float32) ** level_of(streams_of[1], (OCC,), ((0, 64),), -0.2, 0.2), -1.2, -0.3)
    pair_row = touch_ends(jax.random.randint(streams_of[2], (PAIRS,), 0, OCC // N_ROW), jax.random.fold_in(streams_of[2], 1), 0, (OCC // N_ROW) - 1).astype(jnp.int32)
    pair_col = touch_ends(jax.random.randint(streams_of[3], (PAIRS,), 0, OCC // N_COL), jax.random.fold_in(streams_of[3], 1), 0, (OCC // N_COL) - 1).astype(jnp.int32)
    virt_energy = jnp.clip(jnp.exp(math.log(3.0) - 1.7917595 * jax.random.uniform(streams_of[4], (NPNO, PAIRS), jnp.float32) ** level_of(streams_of[4], (NPNO, PAIRS), ((1, 64),), -0.2, 0.2)), 0.5, 3.0)
    amplitudes = centred(streams_of[5], (NPNO, NPNO, PAIRS), 0.3, 1.8, ((2, 64),), jnp.float32)
    intersections = centred(streams_of[6], (NPNO, NPNO, NCPL, PAIRS), NPNO ** -0.5, 1.0, ((2, 4), (3, 64)))
    coupling_fock = jnp.clip(jax.random.uniform(streams_of[7], (NCPL, PAIRS), jnp.float32, -0.25, 0.25) * level_of(streams_of[7], (NCPL, PAIRS), ((0, 4), (1, 64)), -0.4, 0.0), -0.25, 0.25)
    partner_owner_keys = jax.random.split(jax.random.fold_in(streams_of[8], 1), N_FIT * PAIRS // PAIRS_DEV)
    partner_owner_turns = jax.random.permutation(jax.random.fold_in(streams_of[8], 3), N_FIT * PAIRS // PAIRS_DEV)
    partner_owner = jax.vmap(lambda own, number: shared_out(jax.random.fold_in(streams_of[8], 2), own, number, PAIRS_DEV, N_ROW * N_COL, CPL_FIT, CAP, 2))(partner_owner_keys, partner_owner_turns).reshape((N_FIT, PAIRS, CPL_FIT))
    partner_slot = touch_ends(jax.random.randint(streams_of[9], (N_FIT, PAIRS, CPL_FIT), 0, PAIRS_DEV), jax.random.fold_in(streams_of[9], 1), 0, PAIRS_DEV - 1).astype(jnp.int32)
    return dict(orbital_ints=orbital_ints, occ_energy=occ_energy, pair_row=pair_row, pair_col=pair_col, virt_energy=virt_energy, amplitudes=amplitudes, intersections=intersections, coupling_fock=coupling_fock, partner_owner=partner_owner, partner_slot=partner_slot)


def reference(orbital_ints, occ_energy, pair_row, pair_col, virt_energy, amplitudes, intersections, coupling_fock, partner_owner, partner_slot):
    group_count = N_ROW * N_COL
    pair_index = jnp.arange(PAIRS, dtype=jnp.int32)
    group = pair_index // PAIRS_DEV
    row_of = group // N_COL
    col_of = group % N_COL
    first_orb = (row_of * (OCC // N_ROW) + pair_row).astype(jnp.int32)
    second_orb = (((pair_col // OCC_BLK) * N_COL + col_of) * OCC_BLK + pair_col % OCC_BLK).astype(jnp.int32)

    def kernel_group(indices):
        first_ints = orbital_ints[indices[0]].astype(jnp.float32)
        second_ints = orbital_ints[indices[1]].astype(jnp.float32)
        return jnp.einsum("pax,pbx->abp", first_ints, second_ints)

    stacked = lax.map(kernel_group, (first_orb.reshape(group_count, PAIRS_DEV), second_orb.reshape(group_count, PAIRS_DEV)))
    kernel = jnp.transpose(stacked, (1, 2, 0, 3)).reshape(NPNO, NPNO, PAIRS)
    denominator = virt_energy[:, None, :] + virt_energy[None, :, :] - (occ_energy[first_orb] + occ_energy[second_orb])[None, None, :]
    partner = jnp.transpose(partner_owner * PAIRS_DEV + partner_slot, (0, 2, 1)).reshape(NCPL, PAIRS)
    current = amplitudes
    residual = amplitudes
    for turn_index in range(ITERS):
        sent_tiles = current.astype(jnp.bfloat16)
        coupling = jnp.zeros((NPNO, NPNO, PAIRS), jnp.float32)
        for link in range(NCPL):
            tiles = sent_tiles[:, :, partner[link]].astype(jnp.float32)
            intersection = intersections[:, :, link, :].astype(jnp.float32)
            half_product = jnp.einsum("abp,bdp->adp", intersection, tiles).astype(jnp.bfloat16)
            coupled = jnp.einsum("adp,edp->aep", half_product.astype(jnp.float32), intersection)
            coupling = coupling + coupling_fock[link][None, None, :] * coupled
        residual = kernel + denominator * current - coupling
        current = current - residual / denominator
    return current, residual
```

```python
import functools
import math

import jax
import jax.numpy as jnp
from jax import lax
from jax.experimental import pallas as pl
from jax.experimental.pallas import tpu as pltpu
from jax.sharding import PartitionSpec as P

VMEM = pl.BlockSpec(memory_space=pltpu.VMEM)
SMEM = pl.BlockSpec(memory_space=pltpu.SMEM)
F32, BF16, I32 = jnp.float32, jnp.bfloat16, jnp.int32
NT = (((1,), (1,)), ((), ()))
TN = (((0,), (0,)), ((), ()))


def iota(shape, dim):
    return lax.broadcasted_iota(I32, shape, dim)


def request_kernel(cap, owner_ref, slot_ref, energy_ref, payload_ref, target_ref):
    links, pairs = owner_ref.shape
    groups = payload_ref.shape[0]
    before = (iota((pairs, pairs), 0) < iota((pairs, pairs), 1)).astype(BF16)
    base = jnp.zeros((groups, 1), F32)
    payload = jnp.zeros(payload_ref.shape, F32)
    for k in range(links):
        owner = owner_ref[k : k + 1, :]
        slot = slot_ref[k : k + 1, :].astype(F32)
        named = (iota((groups, pairs), 0) == owner).astype(F32)
        count = jnp.dot(named.astype(BF16), before, preferred_element_type=F32) + base
        place = jnp.sum(named * count, axis=0, keepdims=True).astype(I32)
        base = base + jnp.sum(named, axis=1, keepdims=True)
        target_ref[k : k + 1, :] = owner * cap + place
        placed = (iota((payload_ref.shape[1], pairs), 0) == place).astype(BF16)
        payload = payload + lax.dot_general(
            (named * slot).astype(BF16), placed, NT, preferred_element_type=F32
        )
    lane = iota(payload.shape, 1)
    for n in range(energy_ref.shape[0]):
        payload = jnp.where(lane == cap + n, energy_ref[n], payload)
    payload_ref[...] = payload


def gather_kernel(cap, payload_ref, sent_ref, out_ref, low, high):
    groups = payload_ref.shape[0]
    cells, pairs = sent_ref.shape
    slots = payload_ref[...].T.astype(I32)
    half = cap // 2
    for g in range(groups):
        column = slots[:cap, g : g + 1]
        hit = (iota((cap, pairs), 1) == column).astype(F32)
        low[g] = hit[:half]
        high[g] = hit[half:]
    low_hits, high_hits = low[...], high[...]
    hits = jnp.concatenate([low_hits, high_hits], axis=1).reshape(groups * cap, pairs).astype(BF16)
    whole = cells // 128
    for n in range(whole):
        block = lax.dot_general(
            hits, sent_ref[n * 128 : (n + 1) * 128, :], NT, preferred_element_type=F32
        )
        out_ref[:, n * cap : (n + 1) * cap, :] = block.astype(BF16).reshape(groups, cap, 128)
    rest = sent_ref[whole * 128 :, :]
    none = jnp.zeros((128 - rest.shape[0], pairs), BF16)
    low_hits = low_hits.reshape(groups * half, pairs).astype(BF16)
    high_hits = high_hits.reshape(groups * half, pairs).astype(BF16)
    block = lax.dot_general(
        low_hits, jnp.concatenate([rest, none], axis=0), NT, preferred_element_type=F32
    ) + lax.dot_general(
        high_hits, jnp.concatenate([none, rest], axis=0), NT, preferred_element_type=F32
    )
    out_ref[:, whole * cap :, :] = block.astype(BF16).reshape(groups, half, 128)


def select_kernel(cap, target_ref, back_ref, out_ref):
    groups = back_ref.shape[0]
    links, pairs = target_ref.shape
    half = cap // 2
    cells = out_ref.shape[1]
    whole = cells // 128
    rest = cells - whole * 128
    target = jnp.concatenate([target_ref[k : k + 1, :] for k in range(links)], axis=1)
    picks = (iota((groups * cap, links * pairs), 0) == target).astype(BF16)
    for n in range(whole):
        rows = back_ref[:, n * cap : (n + 1) * cap, :].reshape(groups * cap, 128)
        block = lax.dot_general(rows, picks, TN, preferred_element_type=F32).astype(BF16)
        for k in range(links):
            out_ref[k, n * 128 : (n + 1) * 128, :] = block[:, k * pairs : (k + 1) * pairs]
    rows = back_ref[:, whole * cap :, :].reshape(groups * half, 128)
    spot = iota((groups * half, links * pairs), 0)
    spot = (spot // half) * cap + spot % half
    low = lax.dot_general(rows, (spot == target).astype(BF16), TN, preferred_element_type=F32)
    high = lax.dot_general(
        rows, (spot + half == target).astype(BF16), TN, preferred_element_type=F32
    )
    block = (low[:rest] + high[rest:]).astype(BF16)
    for k in range(links):
        out_ref[k, whole * 128 :, :] = block[:, k * pairs : (k + 1) * pairs]


def call(kernel, out_shape, in_specs, scratch=(), flops=0, nbytes=0, many=False):
    return pl.pallas_call(
        kernel,
        out_shape=out_shape,
        in_specs=in_specs,
        out_specs=[VMEM] * len(out_shape) if many else VMEM,
        scratch_shapes=list(scratch),
        compiler_params=pltpu.CompilerParams(vmem_limit_bytes=48 * 2**20),
        cost_estimate=pl.CostEstimate(flops=flops, bytes_accessed=nbytes, transcendentals=0),
    )


def from_everyone(x, axis):
    copies = jnp.broadcast_to(x, (lax.axis_size(axis), *x.shape))
    return lax.all_to_all(copies, axis, split_axis=0, concat_axis=0, tiled=True)


def on_device(
    orbital_ints,
    occ_energy,
    pair_row,
    pair_col,
    virt_energy,
    amplitudes,
    intersections,
    coupling_fock,
    partner_owner,
    partner_slot,
):
    rows, cols = lax.axis_size("row"), lax.axis_size("col")
    groups = rows * cols
    size, _, pairs = amplitudes.shape
    cells = size * size
    links = partner_owner.shape[2]
    cap = 2 * pairs * links // groups
    chunk = cap * cells // 128
    per_block = orbital_ints.shape[0]

    payload, target = call(
        functools.partial(request_kernel, cap),
        [jax.ShapeDtypeStruct((groups, 128), F32), jax.ShapeDtypeStruct((links, pairs), I32)],
        [VMEM, VMEM, SMEM],
        flops=10**7,
        nbytes=10**5,
        many=True,
    )(partner_owner[0].T, partner_slot[0].T, occ_energy)
    incoming = lax.all_to_all(payload, ("row", "col"), split_axis=0, concat_axis=0, tiled=True)

    gather = call(
        functools.partial(gather_kernel, cap),
        jax.ShapeDtypeStruct((groups, chunk, 128), BF16),
        [VMEM, VMEM],
        scratch=[pltpu.VMEM((groups, cap // 2, pairs), F32)] * 2,
        flops=2 * groups * cap * cells * pairs,
        nbytes=2 * groups * cap * cells,
    )
    select = call(
        functools.partial(select_kernel, cap),
        jax.ShapeDtypeStruct((links, cells, pairs), BF16),
        [VMEM, VMEM],
        flops=2 * groups * cap * cells * pairs * links,
        nbytes=4 * groups * cap * cells,
    )

    def exchange(current):
        outgoing = gather(incoming, current.astype(BF16).reshape(cells, pairs))
        returned = lax.all_to_all(
            outgoing, ("row", "col"), split_axis=0, concat_axis=0, tiled=True
        )
        return select(target, returned).reshape(links, size, size, pairs)

    def coupling_of(tiles):
        half_product = jnp.einsum(
            "abcp,cbdp->adcp", intersections, tiles, preferred_element_type=F32
        ).astype(BF16)
        coupled = jnp.einsum(
            "adcp,edcp->aecp", half_product, intersections, preferred_element_type=F32
        )
        return jnp.sum(coupled * coupling_fock[None, None, :, :], axis=2)

    def sum_over_fit(x):
        return from_everyone(x.astype(BF16), "fit").astype(F32).sum(axis=0)

    tiles = exchange(amplitudes)

    row_ints = from_everyone(orbital_ints, "col").reshape(cols * per_block, *orbital_ints.shape[1:])
    col_ints = from_everyone(orbital_ints, "row").reshape(rows * per_block, *orbital_ints.shape[1:])
    kernel = jnp.einsum(
        "pax,pbx->abp",
        row_ints[pair_row],
        col_ints[pair_col],
        preferred_element_type=F32,
    )
    energies = incoming[:, cap : cap + per_block].reshape(rows, cols, per_block)
    row_energy = lax.dynamic_index_in_dim(energies, lax.axis_index("row"), 0, False).reshape(-1)
    col_energy = lax.dynamic_index_in_dim(energies, lax.axis_index("col"), 1, False).reshape(-1)

    def picked(table, index):
        hit = index[None, :] == jnp.arange(table.shape[0], dtype=I32)[:, None]
        return jnp.sum(jnp.where(hit, table[:, None], 0.0), axis=0)

    occupied = picked(row_energy, pair_row) + picked(col_energy, pair_col)
    denominator = virt_energy[:, None, :] + virt_energy[None, :, :] - occupied[None, None, :]

    first = coupling_of(tiles)
    current = sum_over_fit(first - kernel) / denominator
    second = coupling_of(exchange(current))
    residual = sum_over_fit(first - second)
    return (current - residual / denominator, residual)


def solution(mesh):
    placed = (
        P(("row", "col"), None, "fit"),
        P(("row", "col")),
        P(("row", "col")),
        P(("row", "col")),
        P(None, ("row", "col")),
        P(None, None, ("row", "col")),
        P(None, None, "fit", ("row", "col")),
        P("fit", ("row", "col")),
        P("fit", ("row", "col"), None),
        P("fit", ("row", "col"), None),
    )
    return jax.shard_map(
        on_device,
        mesh=mesh,
        in_specs=placed,
        out_specs=(P(None, None, ("row", "col")), P(None, None, ("row", "col"))),
        check_vma=False,
    )
```

```python
import functools

import jax
import jax.numpy as jnp
from jax import lax
from jax.experimental import pallas as pl
from jax.experimental.pallas import tpu as pltpu
from jax.sharding import PartitionSpec as P

VMEM = pl.BlockSpec(memory_space=pltpu.VMEM)
SMEM = pl.BlockSpec(memory_space=pltpu.SMEM)
F32, BF16, I32 = jnp.float32, jnp.bfloat16, jnp.int32
NT = (((1,), (1,)), ((), ()))
TN = (((0,), (0,)), ((), ()))


def iota(shape, dim):
    return lax.broadcasted_iota(I32, shape, dim)


def request_kernel(cap, owner_ref, slot_ref, energy_ref, payload_ref, target_ref):
    links, pairs = owner_ref.shape
    groups = payload_ref.shape[0]
    before = (iota((pairs, pairs), 0) < iota((pairs, pairs), 1)).astype(BF16)
    base = jnp.zeros((groups, 1), F32)
    payload = jnp.zeros(payload_ref.shape, F32)
    for k in range(links):
        owner = owner_ref[k : k + 1, :]
        slot = slot_ref[k : k + 1, :].astype(F32)
        named = (iota((groups, pairs), 0) == owner).astype(F32)
        count = jnp.dot(named.astype(BF16), before, preferred_element_type=F32) + base
        place = jnp.sum(named * count, axis=0, keepdims=True).astype(I32)
        base = base + jnp.sum(named, axis=1, keepdims=True)
        target_ref[k : k + 1, :] = owner * cap + place
        placed = (iota((payload_ref.shape[1], pairs), 0) == place).astype(BF16)
        payload = payload + lax.dot_general(
            (named * slot).astype(BF16), placed, NT, preferred_element_type=F32
        )
    lane = iota(payload.shape, 1)
    for n in range(energy_ref.shape[0]):
        payload = jnp.where(lane == cap + n, energy_ref[n], payload)
    payload_ref[...] = payload


def gather_kernel(cap, payload_ref, sent_ref, out_ref, low, high):
    groups = payload_ref.shape[0]
    cells, pairs = sent_ref.shape
    slots = payload_ref[...].T.astype(I32)
    half = cap // 2
    for g in range(groups):
        column = slots[:cap, g : g + 1]
        hit = (iota((cap, pairs), 1) == column).astype(F32)
        low[g] = hit[:half]
        high[g] = hit[half:]
    low_hits, high_hits = low[...], high[...]
    hits = jnp.concatenate([low_hits, high_hits], axis=1).reshape(groups * cap, pairs).astype(BF16)
    whole = cells // 128
    for n in range(whole):
        block = lax.dot_general(
            hits, sent_ref[n * 128 : (n + 1) * 128, :], NT, preferred_element_type=F32
        )
        out_ref[:, n * cap : (n + 1) * cap, :] = block.astype(BF16).reshape(groups, cap, 128)
    rest = sent_ref[whole * 128 :, :]
    none = jnp.zeros((128 - rest.shape[0], pairs), BF16)
    low_hits = low_hits.reshape(groups * half, pairs).astype(BF16)
    high_hits = high_hits.reshape(groups * half, pairs).astype(BF16)
    block = lax.dot_general(
        low_hits, jnp.concatenate([rest, none], axis=0), NT, preferred_element_type=F32
    ) + lax.dot_general(
        high_hits, jnp.concatenate([none, rest], axis=0), NT, preferred_element_type=F32
    )
    out_ref[:, whole * cap :, :] = block.astype(BF16).reshape(groups, half, 128)


def select_kernel(cap, target_ref, back_ref, out_ref):
    groups = back_ref.shape[0]
    links, pairs = target_ref.shape
    half = cap // 2
    cells = out_ref.shape[1]
    whole = cells // 128
    rest = cells - whole * 128
    target = jnp.concatenate([target_ref[k : k + 1, :] for k in range(links)], axis=1)
    picks = (iota((groups * cap, links * pairs), 0) == target).astype(BF16)
    for n in range(whole):
        rows = back_ref[:, n * cap : (n + 1) * cap, :].reshape(groups * cap, 128)
        block = lax.dot_general(rows, picks, TN, preferred_element_type=F32).astype(BF16)
        for k in range(links):
            out_ref[k, n * 128 : (n + 1) * 128, :] = block[:, k * pairs : (k + 1) * pairs]
    rows = back_ref[:, whole * cap :, :].reshape(groups * half, 128)
    spot = iota((groups * half, links * pairs), 0)
    spot = (spot // half) * cap + spot % half
    low = lax.dot_general(rows, (spot == target).astype(BF16), TN, preferred_element_type=F32)
    high = lax.dot_general(
        rows, (spot + half == target).astype(BF16), TN, preferred_element_type=F32
    )
    block = (low[:rest] + high[rest:]).astype(BF16)
    for k in range(links):
        out_ref[k, whole * 128 :, :] = block[:, k * pairs : (k + 1) * pairs]


def call(kernel, out_shape, in_specs, scratch=(), flops=0, nbytes=0, many=False):
    return pl.pallas_call(
        kernel,
        out_shape=out_shape,
        in_specs=in_specs,
        out_specs=[VMEM] * len(out_shape) if many else VMEM,
        scratch_shapes=list(scratch),
        compiler_params=pltpu.CompilerParams(vmem_limit_bytes=48 * 2**20),
        cost_estimate=pl.CostEstimate(flops=flops, bytes_accessed=nbytes, transcendentals=0),
    )


def from_everyone(x, axis):
    copies = jnp.broadcast_to(x, (lax.axis_size(axis), *x.shape))
    return lax.all_to_all(copies, axis, split_axis=0, concat_axis=0, tiled=True)


def shifted(x, axis, step):
    count = lax.axis_size(axis)
    return lax.ppermute(x, axis, [(n, (n + step) % count) for n in range(count)])


def ring_copies(x, axis, step=1):
    length = lax.axis_size(axis) // step
    ahead, behind = [x], [x]
    for n in range(length // 2):
        ahead.append(shifted(ahead[-1], axis, step))
        if n < length - 1 - length // 2:
            behind.append(shifted(behind[-1], axis, -step))
    return jnp.stack(ahead + behind[:0:-1])


def chip_ring_copies(x, axis):
    count = lax.axis_size(axis)
    mine = ring_copies(x, axis, 2)
    theirs = lax.ppermute(mine, axis, [(n, n ^ 1) for n in range(count)])
    return jnp.concatenate([mine, theirs])


def on_device(
    orbital_ints,
    occ_energy,
    pair_row,
    pair_col,
    virt_energy,
    amplitudes,
    intersections,
    coupling_fock,
    partner_owner,
    partner_slot,
):
    rows, cols = lax.axis_size("row"), lax.axis_size("col")
    groups = rows * cols
    size, _, pairs = amplitudes.shape
    cells = size * size
    links = partner_owner.shape[2]
    cap = 2 * pairs * links // groups
    chunk = cap * cells // 128
    per_block = orbital_ints.shape[0]

    payload, target = call(
        functools.partial(request_kernel, cap),
        [jax.ShapeDtypeStruct((groups, 128), F32), jax.ShapeDtypeStruct((links, pairs), I32)],
        [VMEM, VMEM, SMEM],
        flops=10**7,
        nbytes=10**5,
        many=True,
    )(partner_owner[0].T, partner_slot[0].T, occ_energy)
    incoming = lax.all_to_all(payload, ("row", "col"), split_axis=0, concat_axis=0, tiled=True)

    gather = call(
        functools.partial(gather_kernel, cap),
        jax.ShapeDtypeStruct((groups, chunk, 128), BF16),
        [VMEM, VMEM],
        scratch=[pltpu.VMEM((groups, cap // 2, pairs), F32)] * 2,
        flops=2 * groups * cap * cells * pairs,
        nbytes=2 * groups * cap * cells,
    )
    select = call(
        functools.partial(select_kernel, cap),
        jax.ShapeDtypeStruct((links, cells, pairs), BF16),
        [VMEM, VMEM],
        flops=2 * groups * cap * cells * pairs * links,
        nbytes=4 * groups * cap * cells,
    )

    def returned_tiles(outgoing):
        returned = lax.all_to_all(
            outgoing, ("row", "col"), split_axis=0, concat_axis=0, tiled=True
        )
        return select(target, returned).reshape(links, size, size, pairs)

    def outgoing_tiles(current):
        return gather(incoming, current.astype(BF16).reshape(cells, pairs))

    def coupling_of(tiles):
        half_product = jnp.einsum(
            "abcp,cbdp->adcp", intersections, tiles, preferred_element_type=F32
        ).astype(BF16)
        coupled = jnp.einsum(
            "adcp,edcp->aecp", half_product, intersections, preferred_element_type=F32
        )
        return jnp.sum(coupled * coupling_fock[None, None, :, :], axis=2)

    def sum_over_fit(x):
        return from_everyone(x.astype(BF16), "fit").astype(F32).sum(axis=0)

    outgoing, own_ints = lax.optimization_barrier((outgoing_tiles(amplitudes), orbital_ints))
    tiles = returned_tiles(outgoing)

    row_ints = ring_copies(own_ints, "col").reshape(-1, *orbital_ints.shape[1:])
    col_ints = chip_ring_copies(own_ints, "row").reshape(-1, *orbital_ints.shape[1:])
    owner_col, inner_row = pair_row // per_block, pair_row % per_block
    owner_row, inner_col = pair_col // per_block, pair_col % per_block
    my_row, my_col = lax.axis_index("row"), lax.axis_index("col")
    back = (my_col - owner_col) % cols
    chips_back = (my_row // 2 - owner_row // 2) % (rows // 2)
    other_core = (my_row + owner_row) % 2
    kernel = jnp.einsum(
        "pax,pbx->abp",
        row_ints[back * per_block + inner_row],
        col_ints[(other_core * (rows // 2) + chips_back) * per_block + inner_col],
        preferred_element_type=F32,
    )
    energies = incoming[:, cap : cap + per_block].reshape(rows, cols, per_block)
    row_energy = lax.dynamic_index_in_dim(energies, my_row, 0, False).reshape(-1)
    col_energy = lax.dynamic_index_in_dim(energies, my_col, 1, False).reshape(-1)

    def picked(table, index):
        hit = index[None, :] == jnp.arange(table.shape[0], dtype=I32)[:, None]
        return jnp.sum(jnp.where(hit, table[:, None], 0.0), axis=0)

    occupied = picked(row_energy, pair_row) + picked(col_energy, pair_col)
    denominator = virt_energy[:, None, :] + virt_energy[None, :, :] - occupied[None, None, :]

    first = coupling_of(tiles)
    current = sum_over_fit(first - kernel) / denominator
    second = coupling_of(returned_tiles(outgoing_tiles(current)))
    residual = sum_over_fit(first - second)
    return (current - residual / denominator, residual)


def solution(mesh):
    placed = (
        P(("row", "col"), None, "fit"),
        P(("row", "col")),
        P(("row", "col")),
        P(("row", "col")),
        P(None, ("row", "col")),
        P(None, None, ("row", "col")),
        P(None, None, "fit", ("row", "col")),
        P("fit", ("row", "col")),
        P("fit", ("row", "col"), None),
        P("fit", ("row", "col"), None),
    )
    return jax.shard_map(
        on_device,
        mesh=mesh,
        in_specs=placed,
        out_specs=(P(None, None, ("row", "col")), P(None, None, ("row", "col"))),
        check_vma=False,
    )
```

```python
import functools

import jax
import jax.numpy as jnp
from jax import lax
from jax.experimental import pallas as pl
from jax.experimental.pallas import tpu as pltpu
from jax.sharding import PartitionSpec as P


VMEM = pl.BlockSpec(memory_space=pltpu.VMEM)
SMEM = pl.BlockSpec(memory_space=pltpu.SMEM)
F32, BF16, I32 = jnp.float32, jnp.bfloat16, jnp.int32
NT = (((1,), (1,)), ((), ()))
TN = (((0,), (0,)), ((), ()))


def iota(shape, dim):
    return lax.broadcasted_iota(I32, shape, dim)


def request_kernel(cap, owner_ref, slot_ref, energy_ref, payload_ref, target_ref):
    links, pairs = owner_ref.shape
    groups = payload_ref.shape[0]
    before = (iota((pairs, pairs), 0) < iota((pairs, pairs), 1)).astype(BF16)
    base = jnp.zeros((groups, 1), F32)
    payload = jnp.zeros(payload_ref.shape, F32)
    for k in range(links):
        owner = owner_ref[k : k + 1, :]
        slot = slot_ref[k : k + 1, :].astype(F32)
        named = (iota((groups, pairs), 0) == owner).astype(F32)
        count = jnp.dot(named.astype(BF16), before, preferred_element_type=F32) + base
        place = jnp.sum(named * count, axis=0, keepdims=True).astype(I32)
        base = base + jnp.sum(named, axis=1, keepdims=True)
        target_ref[k : k + 1, :] = owner * cap + place
        placed = (iota((payload_ref.shape[1], pairs), 0) == place).astype(BF16)
        payload = payload + lax.dot_general(
            (named * slot).astype(BF16), placed, NT, preferred_element_type=F32
        )
    lane = iota(payload.shape, 1)
    for n in range(energy_ref.shape[0]):
        payload = jnp.where(lane == cap + n, energy_ref[n], payload)
    payload_ref[...] = payload


def gather_kernel(cap, payload_ref, sent_ref, out_ref, low, high):
    groups = payload_ref.shape[0]
    cells, pairs = sent_ref.shape
    slots = payload_ref[...].T.astype(I32)
    half = cap // 2
    for g in range(groups):
        column = slots[:cap, g : g + 1]
        hit = (iota((cap, pairs), 1) == column).astype(F32)
        low[g] = hit[:half]
        high[g] = hit[half:]
    low_hits, high_hits = low[...], high[...]
    hits = jnp.concatenate([low_hits, high_hits], axis=1).reshape(groups * cap, pairs).astype(BF16)
    whole = cells // 128
    for n in range(whole):
        block = lax.dot_general(
            hits, sent_ref[n * 128 : (n + 1) * 128, :], NT, preferred_element_type=F32
        )
        out_ref[:, n * cap : (n + 1) * cap, :] = block.astype(BF16).reshape(groups, cap, 128)
    rest = sent_ref[whole * 128 :, :]
    none = jnp.zeros((128 - rest.shape[0], pairs), BF16)
    low_hits = low_hits.reshape(groups * half, pairs).astype(BF16)
    high_hits = high_hits.reshape(groups * half, pairs).astype(BF16)
    block = lax.dot_general(
        low_hits, jnp.concatenate([rest, none], axis=0), NT, preferred_element_type=F32
    ) + lax.dot_general(
        high_hits, jnp.concatenate([none, rest], axis=0), NT, preferred_element_type=F32
    )
    out_ref[:, whole * cap :, :] = block.astype(BF16).reshape(groups, half, 128)


def select_kernel(cap, target_ref, back_ref, out_ref):
    groups = back_ref.shape[0]
    links, pairs = target_ref.shape
    half = cap // 2
    cells = out_ref.shape[1]
    whole = cells // 128
    rest = cells - whole * 128
    target = jnp.concatenate([target_ref[k : k + 1, :] for k in range(links)], axis=1)
    picks = (iota((groups * cap, links * pairs), 0) == target).astype(BF16)
    for n in range(whole):
        rows = back_ref[:, n * cap : (n + 1) * cap, :].reshape(groups * cap, 128)
        block = lax.dot_general(rows, picks, TN, preferred_element_type=F32).astype(BF16)
        for k in range(links):
            out_ref[k, n * 128 : (n + 1) * 128, :] = block[:, k * pairs : (k + 1) * pairs]
    rows = back_ref[:, whole * cap :, :].reshape(groups * half, 128)
    spot = iota((groups * half, links * pairs), 0)
    spot = (spot // half) * cap + spot % half
    low = lax.dot_general(rows, (spot == target).astype(BF16), TN, preferred_element_type=F32)
    high = lax.dot_general(
        rows, (spot + half == target).astype(BF16), TN, preferred_element_type=F32
    )
    block = (low[:rest] + high[rest:]).astype(BF16)
    for k in range(links):
        out_ref[k, whole * 128 :, :] = block[:, k * pairs : (k + 1) * pairs]


def call(kernel, out_shape, in_specs, scratch=(), flops=0, nbytes=0, many=False):
    return pl.pallas_call(
        kernel,
        out_shape=out_shape,
        in_specs=in_specs,
        out_specs=[VMEM] * len(out_shape) if many else VMEM,
        scratch_shapes=list(scratch),
        compiler_params=pltpu.CompilerParams(vmem_limit_bytes=48 * 2**20),
        cost_estimate=pl.CostEstimate(flops=flops, bytes_accessed=nbytes, transcendentals=0),
    )


def from_everyone(x, axis):
    copies = jnp.broadcast_to(x, (lax.axis_size(axis), *x.shape))
    return lax.all_to_all(copies, axis, split_axis=0, concat_axis=0, tiled=True)


def shifted(x, axis, step):
    count = lax.axis_size(axis)
    return lax.ppermute(x, axis, [(n, (n + step) % count) for n in range(count)])


def all_copies(x, axis, step=1):
    length = lax.axis_size(axis) // step
    order = sorted(range(1, length), key=lambda n: -min(n, length - n))
    copies = {}
    for n in order:
        copies[n] = shifted(x, axis, n * step)
    return [x] + [copies[n] for n in range(1, length)]


def other_core(x, axis):
    return lax.ppermute(x, axis, [(n, n ^ 1) for n in range(lax.axis_size(axis))])


def whole_step(
    orbital_ints,
    occ_energy,
    pair_row,
    pair_col,
    virt_energy,
    amplitudes,
    intersections,
    coupling_fock,
    partner_owner,
    partner_slot,
):
    rows, cols = lax.axis_size("row"), lax.axis_size("col")
    groups = rows * cols
    size, _, pairs = amplitudes.shape
    cells = size * size
    links = partner_owner.shape[2]
    cap = 2 * pairs * links // groups
    chunk = cap * cells // 128
    per_block = orbital_ints.shape[0]

    make_requests = call(
        functools.partial(request_kernel, cap),
        [jax.ShapeDtypeStruct((groups, 128), F32), jax.ShapeDtypeStruct((links, pairs), I32)],
        [VMEM, VMEM, SMEM],
        flops=10**7,
        nbytes=10**5,
        many=True,
    )
    payload, target = make_requests(partner_owner[0].T, partner_slot[0].T, occ_energy)
    incoming = lax.all_to_all(payload, ("row", "col"), split_axis=0, concat_axis=0, tiled=True)

    gather = call(
        functools.partial(gather_kernel, cap),
        jax.ShapeDtypeStruct((groups, chunk, 128), BF16),
        [VMEM, VMEM],
        scratch=[pltpu.VMEM((groups, cap // 2, pairs), F32)] * 2,
        flops=2 * groups * cap * cells * pairs,
        nbytes=2 * groups * cap * cells,
    )
    select = call(
        functools.partial(select_kernel, cap),
        jax.ShapeDtypeStruct((links, cells, pairs), BF16),
        [VMEM, VMEM],
        flops=2 * groups * cap * cells * pairs * links,
        nbytes=4 * groups * cap * cells,
    )

    def returned_tiles(outgoing):
        returned = lax.all_to_all(
            outgoing, ("row", "col"), split_axis=0, concat_axis=0, tiled=True
        )
        return select(target, returned).reshape(links, size, size, pairs)

    def outgoing_tiles(current):
        return gather(incoming, current.astype(BF16).reshape(cells, pairs))

    def coupling_of(tiles):
        half_product = jnp.einsum(
            "abcp,cbdp->adcp", intersections, tiles, preferred_element_type=F32
        ).astype(BF16)
        coupled = jnp.einsum(
            "adcp,edcp->aecp", half_product, intersections, preferred_element_type=F32
        )
        return jnp.sum(coupled * coupling_fock[None, None, :, :], axis=2)

    def sum_over_fit(x):
        return from_everyone(x.astype(BF16), "fit").astype(F32).sum(axis=0)

    outgoing, row_blocks, chip_blocks = lax.optimization_barrier(
        (
            outgoing_tiles(amplitudes),
            all_copies(orbital_ints, "col"),
            all_copies(orbital_ints, "row", 2),
        )
    )
    tiles = returned_tiles(outgoing)
    row_ints = jnp.concatenate(row_blocks)
    core_ints = jnp.concatenate(chip_blocks)
    col_ints = jnp.concatenate([core_ints, other_core(core_ints, "row")])
    owner_col, inner_row = pair_row // per_block, pair_row % per_block
    owner_row, inner_col = pair_col // per_block, pair_col % per_block
    my_row, my_col = lax.axis_index("row"), lax.axis_index("col")
    back = (my_col - owner_col) % cols
    chips_back = (my_row // 2 - owner_row // 2) % (rows // 2)
    core_off = (my_row + owner_row) % 2
    kernel = jnp.einsum(
        "pax,pbx->abp",
        row_ints[back * per_block + inner_row],
        col_ints[(core_off * (rows // 2) + chips_back) * per_block + inner_col],
        preferred_element_type=F32,
    )
    energies = incoming[:, cap : cap + per_block].reshape(rows, cols, per_block)
    row_energy = lax.dynamic_index_in_dim(energies, my_row, 0, False).reshape(-1)
    col_energy = lax.dynamic_index_in_dim(energies, my_col, 1, False).reshape(-1)

    def picked(table, index):
        hit = index[None, :] == jnp.arange(table.shape[0], dtype=I32)[:, None]
        return jnp.sum(jnp.where(hit, table[:, None], 0.0), axis=0)

    occupied = picked(row_energy, pair_row) + picked(col_energy, pair_col)
    denominator = virt_energy[:, None, :] + virt_energy[None, :, :] - occupied[None, None, :]

    first = coupling_of(tiles)
    current = sum_over_fit(first - kernel) / denominator
    second = coupling_of(returned_tiles(outgoing_tiles(current)))
    residual = sum_over_fit(first - second)
    return (current - residual / denominator, residual)


def solution(mesh):
    placed = (
        P(("row", "col"), None, "fit"),
        P(("row", "col")),
        P(("row", "col")),
        P(("row", "col")),
        P(None, ("row", "col")),
        P(None, None, ("row", "col")),
        P(None, None, "fit", ("row", "col")),
        P("fit", ("row", "col")),
        P("fit", ("row", "col"), None),
        P("fit", ("row", "col"), None),
    )
    return jax.shard_map(
        whole_step,
        mesh=mesh,
        in_specs=placed,
        out_specs=(P(None, None, ("row", "col")), P(None, None, ("row", "col"))),
        check_vma=False,
    )
```

```python
import functools

import jax
import jax.numpy as jnp
from jax import lax
from jax.experimental import pallas as pl
from jax.experimental.pallas import tpu as pltpu
from jax.sharding import PartitionSpec as P


VMEM = pl.BlockSpec(memory_space=pltpu.VMEM)
SMEM = pl.BlockSpec(memory_space=pltpu.SMEM)
F32, BF16, I32 = jnp.float32, jnp.bfloat16, jnp.int32
NT = (((1,), (1,)), ((), ()))
TN = (((0,), (0,)), ((), ()))


def iota(shape, dim):
    return lax.broadcasted_iota(I32, shape, dim)


def request_kernel(cap, owner_ref, slot_ref, energy_ref, payload_ref, target_ref):
    links, pairs = owner_ref.shape
    groups = payload_ref.shape[0]
    before = (iota((pairs, pairs), 0) < iota((pairs, pairs), 1)).astype(BF16)
    base = jnp.zeros((groups, 1), F32)
    payload = jnp.zeros(payload_ref.shape, F32)
    for k in range(links):
        owner = owner_ref[k : k + 1, :]
        slot = slot_ref[k : k + 1, :].astype(F32)
        named = (iota((groups, pairs), 0) == owner).astype(F32)
        count = jnp.dot(named.astype(BF16), before, preferred_element_type=F32) + base
        place = jnp.sum(named * count, axis=0, keepdims=True).astype(I32)
        base = base + jnp.sum(named, axis=1, keepdims=True)
        target_ref[k : k + 1, :] = owner * cap + place
        placed = (iota((payload_ref.shape[1], pairs), 0) == place).astype(BF16)
        payload = payload + lax.dot_general(
            (named * slot).astype(BF16), placed, NT, preferred_element_type=F32
        )
    lane = iota(payload.shape, 1)
    for n in range(energy_ref.shape[0]):
        payload = jnp.where(lane == cap + n, energy_ref[n], payload)
    payload_ref[...] = payload


def gather_kernel(cap, payload_ref, sent_ref, out_ref, low, high):
    groups = payload_ref.shape[0]
    cells, pairs = sent_ref.shape
    slots = payload_ref[...].T.astype(I32)
    half = cap // 2
    for g in range(groups):
        column = slots[:cap, g : g + 1]
        hit = (iota((cap, pairs), 1) == column).astype(F32)
        low[g] = hit[:half]
        high[g] = hit[half:]
    low_hits, high_hits = low[...], high[...]
    hits = jnp.concatenate([low_hits, high_hits], axis=1).reshape(groups * cap, pairs).astype(BF16)
    whole = cells // 128

    def some_blocks(turn, carry):
        for m in range(3):
            n = turn * 3 + m
            block = lax.dot_general(
                hits,
                sent_ref[pl.ds(pl.multiple_of(n * 128, 128), 128), :],
                NT,
                preferred_element_type=F32,
            )
            here = pl.ds(pl.multiple_of(n * cap, cap), cap)
            out_ref[:, here, :] = block.astype(BF16).reshape(groups, cap, 128)
        return carry

    lax.fori_loop(0, whole // 3, some_blocks, 0)
    for n in range(whole // 3 * 3, whole):
        some = lax.dot_general(
            hits, sent_ref[n * 128 : (n + 1) * 128, :], NT, preferred_element_type=F32
        )
        out_ref[:, n * cap : (n + 1) * cap, :] = some.astype(BF16).reshape(groups, cap, 128)
    rest = sent_ref[whole * 128 :, :]
    none = jnp.zeros((128 - rest.shape[0], pairs), BF16)
    low_hits = low_hits.reshape(groups * half, pairs).astype(BF16)
    high_hits = high_hits.reshape(groups * half, pairs).astype(BF16)
    block = lax.dot_general(
        low_hits, jnp.concatenate([rest, none], axis=0), NT, preferred_element_type=F32
    ) + lax.dot_general(
        high_hits, jnp.concatenate([none, rest], axis=0), NT, preferred_element_type=F32
    )
    out_ref[:, whole * cap :, :] = block.astype(BF16).reshape(groups, half, 128)


def select_kernel(cap, target_ref, back_ref, out_ref):
    groups = back_ref.shape[0]
    links, pairs = target_ref.shape
    half = cap // 2
    cells = out_ref.shape[1]
    whole = cells // 128
    rest = cells - whole * 128
    target = jnp.concatenate([target_ref[k : k + 1, :] for k in range(links)], axis=1)
    picks = (iota((groups * cap, links * pairs), 0) == target).astype(BF16)
    for n in range(whole):
        rows = back_ref[:, n * cap : (n + 1) * cap, :].reshape(groups * cap, 128)
        block = lax.dot_general(rows, picks, TN, preferred_element_type=F32).astype(BF16)
        for k in range(links):
            out_ref[k, n * 128 : (n + 1) * 128, :] = block[:, k * pairs : (k + 1) * pairs]
    rows = back_ref[:, whole * cap :, :].reshape(groups * half, 128)
    spot = iota((groups * half, links * pairs), 0)
    spot = (spot // half) * cap + spot % half
    low = lax.dot_general(rows, (spot == target).astype(BF16), TN, preferred_element_type=F32)
    high = lax.dot_general(
        rows, (spot + half == target).astype(BF16), TN, preferred_element_type=F32
    )
    block = (low[:rest] + high[rest:]).astype(BF16)
    for k in range(links):
        out_ref[k, whole * 128 :, :] = block[:, k * pairs : (k + 1) * pairs]


def stacked_kernel(*refs):
    *blocks, out_ref = refs
    count = blocks[0].shape[0]
    for n, block in enumerate(blocks):
        out_ref[n * count : (n + 1) * count] = block[...]


def rounded_kernel(x_ref, y_ref, low_ref, high_ref):
    half = low_ref.shape[0]
    low_ref[...] = (x_ref[:half] - y_ref[:half]).astype(BF16)
    high_ref[...] = (x_ref[half:] - y_ref[half:]).astype(BF16)


def added_kernel(low_ref, high_ref, low_there, high_there, low_out, high_out):
    low_out[...] = (low_ref[...].astype(F32) + low_there[...].astype(F32)).astype(BF16)
    high_out[...] = (high_ref[...].astype(F32) + high_there[...].astype(F32)).astype(BF16)


def joined_kernel(low_ref, high_ref, low_there, high_there, out_ref):
    half = low_ref.shape[0]
    out_ref[:half] = low_ref[...].astype(F32) + low_there[...].astype(F32)
    out_ref[half:] = high_ref[...].astype(F32) + high_there[...].astype(F32)


def call(kernel, out_shape, in_specs, scratch=(), flops=0, nbytes=0, many=False):
    return pl.pallas_call(
        kernel,
        out_shape=out_shape,
        in_specs=in_specs,
        out_specs=[VMEM] * len(out_shape) if many else VMEM,
        scratch_shapes=list(scratch),
        compiler_params=pltpu.CompilerParams(vmem_limit_bytes=48 * 2**20),
        cost_estimate=pl.CostEstimate(flops=flops, bytes_accessed=nbytes, transcendentals=0),
    )


def stacked(blocks):
    first, *shape = blocks[0].shape
    whole = jax.ShapeDtypeStruct((len(blocks) * first, *shape), blocks[0].dtype)
    return call(stacked_kernel, whole, [VMEM] * len(blocks), nbytes=2 * 10**6)(*blocks)


def shifted(x, axis, step):
    count = lax.axis_size(axis)
    return lax.ppermute(x, axis, [(n, (n + step) % count) for n in range(count)])


def all_copies(x, axis, step=1):
    length = lax.axis_size(axis) // step
    order = sorted(range(1, length), key=lambda n: -min(n, length - n))
    copies = {}
    for n in order:
        copies[n] = shifted(x, axis, n * step)
    return [x] + [copies[n] for n in range(1, length)]


def other_core(x, axis):
    return lax.ppermute(x, axis, [(n, n ^ 1) for n in range(lax.axis_size(axis))])


def whole_step(
    orbital_ints,
    occ_energy,
    pair_row,
    pair_col,
    virt_energy,
    amplitudes,
    intersections,
    coupling_fock,
    partner_owner,
    partner_slot,
):
    rows, cols = lax.axis_size("row"), lax.axis_size("col")
    groups = rows * cols
    size, _, pairs = amplitudes.shape
    cells = size * size
    links = partner_owner.shape[2]
    cap = 2 * pairs * links // groups
    chunk = cap * cells // 128
    per_block = orbital_ints.shape[0]

    make_requests = call(
        functools.partial(request_kernel, cap),
        [jax.ShapeDtypeStruct((groups, 128), F32), jax.ShapeDtypeStruct((links, pairs), I32)],
        [VMEM, VMEM, SMEM],
        flops=10**7,
        nbytes=10**5,
        many=True,
    )
    payload, target = make_requests(partner_owner[0].T, partner_slot[0].T, occ_energy)
    incoming = lax.all_to_all(payload, ("row", "col"), split_axis=0, concat_axis=0, tiled=True)

    gather = call(
        functools.partial(gather_kernel, cap),
        jax.ShapeDtypeStruct((groups, chunk, 128), BF16),
        [VMEM, VMEM],
        scratch=[pltpu.VMEM((groups, cap // 2, pairs), F32)] * 2,
        flops=2 * groups * cap * cells * pairs,
        nbytes=2 * groups * cap * cells,
    )
    select = call(
        functools.partial(select_kernel, cap),
        jax.ShapeDtypeStruct((links, cells, pairs), BF16),
        [VMEM, VMEM],
        flops=2 * groups * cap * cells * pairs * links,
        nbytes=4 * groups * cap * cells,
    )

    def returned_tiles(outgoing):
        returned = lax.all_to_all(
            outgoing, ("row", "col"), split_axis=0, concat_axis=0, tiled=True
        )
        return select(target, returned).reshape(links, size, size, pairs)

    def outgoing_tiles(current):
        return gather(incoming, current.astype(BF16).reshape(cells, pairs))

    def coupling_of(tiles):
        half_product = jnp.einsum(
            "abcp,cbdp->adcp", intersections, tiles, preferred_element_type=F32
        ).astype(BF16)
        coupled = jnp.einsum(
            "adcp,edcp->aecp", half_product, intersections, preferred_element_type=F32
        )
        return jnp.sum(coupled * coupling_fock[None, None, :, :], axis=2)

    def sum_over_fit(x, y):
        count = lax.axis_size("fit")
        sides = [(n, n ^ 1) for n in range(count)], [(n, count - 1 - n) for n in range(count)]
        part = jax.ShapeDtypeStruct((cells // 2, pairs), BF16)
        halves = call(rounded_kernel, [part] * 2, [VMEM] * 2, nbytes=10**6, many=True)(
            x.reshape(cells, pairs), y.reshape(cells, pairs)
        )
        for turn in range(2):
            there = [lax.ppermute(h, "fit", sides[n ^ turn]) for n, h in enumerate(halves)]
            if turn == 0:
                halves = call(added_kernel, [part] * 2, [VMEM] * 4, nbytes=10**6, many=True)(
                    *halves, *there
                )
        whole = jax.ShapeDtypeStruct((cells, pairs), F32)
        return call(joined_kernel, whole, [VMEM] * 4, nbytes=10**6)(*halves, *there).reshape(
            size, size, pairs
        )

    outgoing, row_blocks, chip_blocks = lax.optimization_barrier(
        (
            outgoing_tiles(amplitudes),
            all_copies(orbital_ints, "col"),
            all_copies(orbital_ints, "row", 2),
        )
    )
    tiles = returned_tiles(outgoing)
    row_ints = stacked(row_blocks)
    core_ints = stacked(chip_blocks)
    col_ints = stacked([core_ints, other_core(core_ints, "row")])
    owner_col, inner_row = pair_row // per_block, pair_row % per_block
    owner_row, inner_col = pair_col // per_block, pair_col % per_block
    my_row, my_col = lax.axis_index("row"), lax.axis_index("col")
    back = (my_col - owner_col) % cols
    chips_back = (my_row // 2 - owner_row // 2) % (rows // 2)
    core_off = (my_row + owner_row) % 2
    kernel = jnp.einsum(
        "pax,pbx->abp",
        row_ints[back * per_block + inner_row],
        col_ints[(core_off * (rows // 2) + chips_back) * per_block + inner_col],
        preferred_element_type=F32,
    )
    energies = incoming[:, cap : cap + per_block].reshape(rows, cols, per_block)
    row_energy = lax.dynamic_index_in_dim(energies, my_row, 0, False).reshape(-1)
    col_energy = lax.dynamic_index_in_dim(energies, my_col, 1, False).reshape(-1)

    def picked(table, index):
        hit = index[None, :] == jnp.arange(table.shape[0], dtype=I32)[:, None]
        return jnp.sum(jnp.where(hit, table[:, None], 0.0), axis=0)

    occupied = picked(row_energy, pair_row) + picked(col_energy, pair_col)
    denominator = virt_energy[:, None, :] + virt_energy[None, :, :] - occupied[None, None, :]

    first = coupling_of(tiles)
    current = sum_over_fit(first, kernel) / denominator
    second = coupling_of(returned_tiles(outgoing_tiles(current)))
    residual = sum_over_fit(first, second)
    return (current - residual / denominator, residual)


def solution(mesh):
    placed = (
        P(("row", "col"), None, "fit"),
        P(("row", "col")),
        P(("row", "col")),
        P(("row", "col")),
        P(None, ("row", "col")),
        P(None, None, ("row", "col")),
        P(None, None, "fit", ("row", "col")),
        P("fit", ("row", "col")),
        P("fit", ("row", "col"), None),
        P("fit", ("row", "col"), None),
    )
    return jax.shard_map(
        whole_step,
        mesh=mesh,
        in_specs=placed,
        out_specs=(P(None, None, ("row", "col")), P(None, None, ("row", "col"))),
        check_vma=False,
    )
```

```python
import functools

import jax
import jax.numpy as jnp
from jax import lax
from jax.experimental import pallas as pl
from jax.experimental.pallas import tpu as pltpu
from jax.sharding import PartitionSpec as P


VMEM = pl.BlockSpec(memory_space=pltpu.VMEM)
SMEM = pl.BlockSpec(memory_space=pltpu.SMEM)
F32, BF16, I32 = jnp.float32, jnp.bfloat16, jnp.int32
NT = (((1,), (1,)), ((), ()))
TN = (((0,), (0,)), ((), ()))


def iota(shape, dim):
    return lax.broadcasted_iota(I32, shape, dim)


def request_kernel(cap, owner_ref, slot_ref, energy_ref, payload_ref, target_ref):
    links, pairs = owner_ref.shape
    groups = payload_ref.shape[0]
    before = (iota((pairs, pairs), 0) < iota((pairs, pairs), 1)).astype(BF16)
    base = jnp.zeros((groups, 1), F32)
    payload = jnp.zeros(payload_ref.shape, F32)
    for k in range(links):
        owner = owner_ref[k : k + 1, :]
        slot = slot_ref[k : k + 1, :].astype(F32)
        named = (iota((groups, pairs), 0) == owner).astype(F32)
        count = jnp.dot(named.astype(BF16), before, preferred_element_type=F32) + base
        place = jnp.sum(named * count, axis=0, keepdims=True).astype(I32)
        base = base + jnp.sum(named, axis=1, keepdims=True)
        target_ref[k : k + 1, :] = owner * cap + place
        placed = (iota((payload_ref.shape[1], pairs), 0) == place).astype(BF16)
        payload = payload + lax.dot_general(
            (named * slot).astype(BF16), placed, NT, preferred_element_type=F32
        )
    lane = iota(payload.shape, 1)
    for n in range(energy_ref.shape[0]):
        payload = jnp.where(lane == cap + n, energy_ref[n], payload)
    payload_ref[...] = payload


def gather_kernel(cap, payload_ref, sent_ref, out_ref, low, high):
    groups = payload_ref.shape[0]
    cells, pairs = sent_ref.shape
    slots = payload_ref[...].T.astype(I32)
    half = cap // 2
    for g in range(groups):
        column = slots[:cap, g : g + 1]
        hit = (iota((cap, pairs), 1) == column).astype(F32)
        low[g] = hit[:half]
        high[g] = hit[half:]
    low_hits, high_hits = low[...], high[...]
    hits = jnp.concatenate([low_hits, high_hits], axis=1).reshape(groups * cap, pairs).astype(BF16)
    whole = cells // 128
    for n in range(whole):
        block = lax.dot_general(
            hits, sent_ref[n * 128 : (n + 1) * 128, :].astype(BF16), NT, preferred_element_type=F32
        )
        out_ref[:, n * cap : (n + 1) * cap, :] = block.astype(BF16).reshape(groups, cap, 128)
    rest = sent_ref[whole * 128 :, :].astype(BF16)
    none = jnp.zeros((128 - rest.shape[0], pairs), BF16)
    low_hits = low_hits.reshape(groups * half, pairs).astype(BF16)
    high_hits = high_hits.reshape(groups * half, pairs).astype(BF16)
    block = lax.dot_general(
        low_hits, jnp.concatenate([rest, none], axis=0), NT, preferred_element_type=F32
    ) + lax.dot_general(
        high_hits, jnp.concatenate([none, rest], axis=0), NT, preferred_element_type=F32
    )
    out_ref[:, whole * cap :, :] = block.astype(BF16).reshape(groups, half, 128)


def select_kernel(cap, target_ref, back_ref, out_ref):
    groups = back_ref.shape[0]
    links, pairs = target_ref.shape
    half = cap // 2
    cells = out_ref.shape[1]
    whole = cells // 128
    rest = cells - whole * 128
    target = jnp.concatenate([target_ref[k : k + 1, :] for k in range(links)], axis=1)
    picks = (iota((groups * cap, links * pairs), 0) == target).astype(BF16)
    for n in range(whole):
        rows = back_ref[:, n * cap : (n + 1) * cap, :].reshape(groups * cap, 128)
        block = lax.dot_general(rows, picks, TN, preferred_element_type=F32).astype(BF16)
        for k in range(links):
            out_ref[k, n * 128 : (n + 1) * 128, :] = block[:, k * pairs : (k + 1) * pairs]
    rows = back_ref[:, whole * cap :, :].reshape(groups * half, 128)
    spot = iota((groups * half, links * pairs), 0)
    spot = (spot // half) * cap + spot % half
    low = lax.dot_general(rows, (spot == target).astype(BF16), TN, preferred_element_type=F32)
    high = lax.dot_general(
        rows, (spot + half == target).astype(BF16), TN, preferred_element_type=F32
    )
    block = (low[:rest] + high[rest:]).astype(BF16)
    for k in range(links):
        out_ref[k, whole * 128 :, :] = block[:, k * pairs : (k + 1) * pairs]


def stacked_kernel(*refs):
    *blocks, out_ref = refs
    count = blocks[0].shape[0]
    for n, block in enumerate(blocks):
        out_ref[n * count : (n + 1) * count] = block[...]


def halved_kernel(x_ref, low_ref, high_ref):
    half = low_ref.shape[0]
    low_ref[...] = x_ref[:half]
    high_ref[...] = x_ref[half:]


def added_kernel(low_ref, high_ref, low_there, high_there, low_out, high_out):
    low_out[...] = (low_ref[...].astype(F32) + low_there[...].astype(F32)).astype(BF16)
    high_out[...] = (high_ref[...].astype(F32) + high_there[...].astype(F32)).astype(BF16)


def joined_kernel(low_ref, high_ref, low_there, high_there, out_ref):
    half = low_ref.shape[0]
    out_ref[:half] = low_ref[...].astype(F32) + low_there[...].astype(F32)
    out_ref[half:] = high_ref[...].astype(F32) + high_there[...].astype(F32)


def call(kernel, out_shape, in_specs, scratch=(), flops=0, nbytes=0, many=False, grant=6):
    return pl.pallas_call(
        kernel,
        out_shape=out_shape,
        in_specs=in_specs,
        out_specs=[VMEM] * len(out_shape) if many else VMEM,
        scratch_shapes=list(scratch),
        compiler_params=pltpu.CompilerParams(vmem_limit_bytes=grant * 2**20),
        cost_estimate=pl.CostEstimate(flops=flops, bytes_accessed=nbytes, transcendentals=0),
    )


def stacked(blocks):
    first, *shape = blocks[0].shape
    whole = jax.ShapeDtypeStruct((len(blocks) * first, *shape), blocks[0].dtype)
    return call(stacked_kernel, whole, [VMEM] * len(blocks), nbytes=2 * 10**6)(*blocks)


def shifted(x, axis, step):
    count = lax.axis_size(axis)
    return lax.ppermute(x, axis, [(n, (n + step) % count) for n in range(count)])


def all_copies(x, axis, step=1):
    length = lax.axis_size(axis) // step
    order = sorted(range(1, length), key=lambda n: -min(n, length - n))
    copies = {}
    for n in order:
        copies[n] = shifted(x, axis, n * step)
    return [x] + [copies[n] for n in range(1, length)]


def other_core(x, axis):
    return lax.ppermute(x, axis, [(n, n ^ 1) for n in range(lax.axis_size(axis))])


def whole_step(
    orbital_ints,
    occ_energy,
    pair_row,
    pair_col,
    virt_energy,
    amplitudes,
    intersections,
    coupling_fock,
    partner_owner,
    partner_slot,
):
    rows, cols = lax.axis_size("row"), lax.axis_size("col")
    groups = rows * cols
    size, _, pairs = amplitudes.shape
    cells = size * size
    links = partner_owner.shape[2]
    cap = 2 * pairs * links // groups
    chunk = cap * cells // 128
    per_block = orbital_ints.shape[0]

    make_requests = call(
        functools.partial(request_kernel, cap),
        [jax.ShapeDtypeStruct((groups, 128), F32), jax.ShapeDtypeStruct((links, pairs), I32)],
        [VMEM, VMEM, SMEM],
        flops=10**7,
        nbytes=10**5,
        many=True,
    )
    payload, target = make_requests(partner_owner[0].T, partner_slot[0].T, occ_energy)
    incoming = lax.all_to_all(payload, ("row", "col"), split_axis=0, concat_axis=0, tiled=True)

    gather = call(
        functools.partial(gather_kernel, cap),
        jax.ShapeDtypeStruct((groups, chunk, 128), BF16),
        [VMEM, VMEM],
        scratch=[pltpu.VMEM((groups, cap // 2, pairs), F32)] * 2,
        flops=2 * groups * cap * cells * pairs,
        nbytes=2 * groups * cap * cells,
        grant=14,
    )
    select = call(
        functools.partial(select_kernel, cap),
        jax.ShapeDtypeStruct((links, cells, pairs), BF16),
        [VMEM, VMEM],
        flops=2 * groups * cap * cells * pairs * links,
        nbytes=4 * groups * cap * cells,
        grant=14,
    )

    def returned_tiles(outgoing):
        returned = lax.all_to_all(
            outgoing, ("row", "col"), split_axis=0, concat_axis=0, tiled=True
        )
        return select(target, returned).reshape(links, size, size, pairs)

    def outgoing_tiles(current):
        return gather(incoming, current.reshape(cells, pairs))

    def coupling_of(tiles):
        half_product = jnp.einsum(
            "abcp,cbdp->adcp", intersections, tiles, preferred_element_type=F32
        ).astype(BF16)
        coupled = jnp.einsum(
            "adcp,edcp->aecp", half_product, intersections, preferred_element_type=F32
        )
        return jnp.sum(coupled * coupling_fock[None, None, :, :], axis=2)

    def sum_over_fit(x, y):
        count = lax.axis_size("fit")
        sides = [(n, n ^ 1) for n in range(count)], [(n, count - 1 - n) for n in range(count)]
        part = jax.ShapeDtypeStruct((cells // 2, pairs), BF16)
        halves = call(halved_kernel, [part] * 2, [VMEM], nbytes=10**6, many=True)(
            (x - y).astype(BF16).reshape(cells, pairs)
        )
        for turn in range(2):
            there = [lax.ppermute(h, "fit", sides[n ^ turn]) for n, h in enumerate(halves)]
            if turn == 0:
                halves = call(added_kernel, [part] * 2, [VMEM] * 4, nbytes=10**6, many=True)(
                    *halves, *there
                )
        whole = jax.ShapeDtypeStruct((cells, pairs), F32)
        return call(joined_kernel, whole, [VMEM] * 4, nbytes=10**6)(*halves, *there).reshape(
            size, size, pairs
        )

    outgoing, row_blocks, chip_blocks = lax.optimization_barrier(
        (
            outgoing_tiles(amplitudes),
            all_copies(orbital_ints, "col"),
            all_copies(orbital_ints, "row", 2),
        )
    )
    tiles = returned_tiles(outgoing)
    row_ints = stacked(row_blocks)
    core_ints = stacked(chip_blocks)
    col_ints = stacked([core_ints, other_core(core_ints, "row")])
    owner_col, inner_row = pair_row // per_block, pair_row % per_block
    owner_row, inner_col = pair_col // per_block, pair_col % per_block
    my_row, my_col = lax.axis_index("row"), lax.axis_index("col")
    back = (my_col - owner_col) % cols
    chips_back = (my_row // 2 - owner_row // 2) % (rows // 2)
    core_off = (my_row + owner_row) % 2
    kernel = jnp.einsum(
        "pax,pbx->abp",
        row_ints[back * per_block + inner_row],
        col_ints[(core_off * (rows // 2) + chips_back) * per_block + inner_col],
        preferred_element_type=F32,
    )
    energies = incoming[:, cap : cap + per_block].reshape(rows, cols, per_block)
    row_energy = lax.dynamic_index_in_dim(energies, my_row, 0, False).reshape(-1)
    col_energy = lax.dynamic_index_in_dim(energies, my_col, 1, False).reshape(-1)

    def picked(table, index):
        hit = index[None, :] == jnp.arange(table.shape[0], dtype=I32)[:, None]
        return jnp.sum(jnp.where(hit, table[:, None], 0.0), axis=0)

    occupied = picked(row_energy, pair_row) + picked(col_energy, pair_col)
    denominator = virt_energy[:, None, :] + virt_energy[None, :, :] - occupied[None, None, :]

    first = coupling_of(tiles)
    current = sum_over_fit(first, kernel) / denominator
    second = coupling_of(returned_tiles(outgoing_tiles(current)))
    residual = sum_over_fit(first, second)
    return (current - residual / denominator, residual)


def solution(mesh):
    placed = (
        P(("row", "col"), None, "fit"),
        P(("row", "col")),
        P(("row", "col")),
        P(("row", "col")),
        P(None, ("row", "col")),
        P(None, None, ("row", "col")),
        P(None, None, "fit", ("row", "col")),
        P("fit", ("row", "col")),
        P("fit", ("row", "col"), None),
        P("fit", ("row", "col"), None),
    )
    return jax.shard_map(
        whole_step,
        mesh=mesh,
        in_specs=placed,
        out_specs=(P(None, None, ("row", "col")), P(None, None, ("row", "col"))),
        check_vma=False,
    )
```

```python
import functools

import jax
import jax.numpy as jnp
from jax import lax
from jax.experimental import pallas as pl
from jax.experimental.pallas import tpu as pltpu
from jax.sharding import PartitionSpec as P


VMEM = pl.BlockSpec(memory_space=pltpu.VMEM)
SMEM = pl.BlockSpec(memory_space=pltpu.SMEM)
F32, BF16, I32 = jnp.float32, jnp.bfloat16, jnp.int32
NT = (((1,), (1,)), ((), ()))
TN = (((0,), (0,)), ((), ()))


def iota(shape, dim):
    return lax.broadcasted_iota(I32, shape, dim)


def request_kernel(cap, owner_ref, slot_ref, energy_ref, payload_ref, target_ref):
    links, pairs = owner_ref.shape
    groups = payload_ref.shape[0]
    before = (iota((pairs, pairs), 0) < iota((pairs, pairs), 1)).astype(BF16)
    base = jnp.zeros((groups, 1), F32)
    payload = jnp.zeros(payload_ref.shape, F32)
    for k in range(links):
        owner = owner_ref[k : k + 1, :]
        slot = slot_ref[k : k + 1, :].astype(F32)
        named = (iota((groups, pairs), 0) == owner).astype(F32)
        count = jnp.dot(named.astype(BF16), before, preferred_element_type=F32) + base
        place = jnp.sum(named * count, axis=0, keepdims=True).astype(I32)
        base = base + jnp.sum(named, axis=1, keepdims=True)
        target_ref[k : k + 1, :] = owner * cap + place
        placed = (iota((payload_ref.shape[1], pairs), 0) == place).astype(BF16)
        payload = payload + lax.dot_general(
            (named * slot).astype(BF16), placed, NT, preferred_element_type=F32
        )
    lane = iota(payload.shape, 1)
    for n in range(energy_ref.shape[0]):
        payload = jnp.where(lane == cap + n, energy_ref[n], payload)
    payload_ref[...] = payload


def gather_kernel(cap, payload_ref, sent_ref, out_ref, low, high):
    groups = payload_ref.shape[0]
    cells, pairs = sent_ref.shape
    slots = payload_ref[...].T.astype(I32)
    half = cap // 2
    for g in range(groups):
        column = slots[:cap, g : g + 1]
        hit = (iota((cap, pairs), 1) == column).astype(F32)
        low[g] = hit[:half]
        high[g] = hit[half:]
    low_hits, high_hits = low[...], high[...]
    hits = jnp.concatenate([low_hits, high_hits], axis=1).reshape(groups * cap, pairs).astype(BF16)
    whole = cells // 128
    for n in range(whole):
        block = lax.dot_general(
            hits, sent_ref[n * 128 : (n + 1) * 128, :].astype(BF16), NT, preferred_element_type=F32
        )
        out_ref[:, n * cap : (n + 1) * cap, :] = block.astype(BF16).reshape(groups, cap, 128)
    rest = sent_ref[whole * 128 :, :].astype(BF16)
    none = jnp.zeros((128 - rest.shape[0], pairs), BF16)
    low_hits = low_hits.reshape(groups * half, pairs).astype(BF16)
    high_hits = high_hits.reshape(groups * half, pairs).astype(BF16)
    block = lax.dot_general(
        low_hits, jnp.concatenate([rest, none], axis=0), NT, preferred_element_type=F32
    ) + lax.dot_general(
        high_hits, jnp.concatenate([none, rest], axis=0), NT, preferred_element_type=F32
    )
    out_ref[:, whole * cap :, :] = block.astype(BF16).reshape(groups, half, 128)


def select_kernel(cap, target_ref, back_ref, out_ref):
    groups = back_ref.shape[0]
    links, pairs = target_ref.shape
    half = cap // 2
    cells = out_ref.shape[1]
    whole = cells // 128
    rest = cells - whole * 128
    target = jnp.concatenate([target_ref[k : k + 1, :] for k in range(links)], axis=1)
    picks = (iota((groups * cap, links * pairs), 0) == target).astype(BF16)
    for n in range(whole):
        rows = back_ref[:, n * cap : (n + 1) * cap, :].reshape(groups * cap, 128)
        block = lax.dot_general(rows, picks, TN, preferred_element_type=F32).astype(BF16)
        for k in range(links):
            out_ref[k, n * 128 : (n + 1) * 128, :] = block[:, k * pairs : (k + 1) * pairs]
    rows = back_ref[:, whole * cap :, :].reshape(groups * half, 128)
    spot = iota((groups * half, links * pairs), 0)
    spot = (spot // half) * cap + spot % half
    low = lax.dot_general(rows, (spot == target).astype(BF16), TN, preferred_element_type=F32)
    high = lax.dot_general(
        rows, (spot + half == target).astype(BF16), TN, preferred_element_type=F32
    )
    block = (low[:rest] + high[rest:]).astype(BF16)
    for k in range(links):
        out_ref[k, whole * 128 :, :] = block[:, k * pairs : (k + 1) * pairs]


def stacked_kernel(*refs):
    *blocks, out_ref = refs
    count = blocks[0].shape[0]
    for n, block in enumerate(blocks):
        out_ref[n * count : (n + 1) * count] = block[...]


def rounded_kernel(x_ref, y_ref, low_ref, high_ref):
    half = low_ref.shape[0]
    low_ref[...] = (x_ref[:half] - y_ref[:half]).astype(BF16)
    high_ref[...] = (x_ref[half:] - y_ref[half:]).astype(BF16)


def added_kernel(low_ref, high_ref, low_there, high_there, low_out, high_out):
    low_out[...] = (low_ref[...].astype(F32) + low_there[...].astype(F32)).astype(BF16)
    high_out[...] = (high_ref[...].astype(F32) + high_there[...].astype(F32)).astype(BF16)


def joined_kernel(low_ref, high_ref, low_there, high_there, out_ref):
    half = low_ref.shape[0]
    out_ref[:half] = low_ref[...].astype(F32) + low_there[...].astype(F32)
    out_ref[half:] = high_ref[...].astype(F32) + high_there[...].astype(F32)


def call(kernel, out_shape, in_specs, scratch=(), flops=0, nbytes=0, many=False, grant=6):
    return pl.pallas_call(
        kernel,
        out_shape=out_shape,
        in_specs=in_specs,
        out_specs=[VMEM] * len(out_shape) if many else VMEM,
        scratch_shapes=list(scratch),
        compiler_params=pltpu.CompilerParams(vmem_limit_bytes=grant * 2**20),
        cost_estimate=pl.CostEstimate(flops=flops, bytes_accessed=nbytes, transcendentals=0),
    )


def stacked(blocks):
    first, *shape = blocks[0].shape
    whole = jax.ShapeDtypeStruct((len(blocks) * first, *shape), blocks[0].dtype)
    return call(stacked_kernel, whole, [VMEM] * len(blocks), nbytes=2 * 10**6)(*blocks)


def shifted(x, axis, step):
    count = lax.axis_size(axis)
    return lax.ppermute(x, axis, [(n, (n + step) % count) for n in range(count)])


def all_copies(x, axis, step=1):
    length = lax.axis_size(axis) // step
    order = sorted(range(1, length), key=lambda n: -min(n, length - n))
    copies = {}
    for n in order:
        copies[n] = shifted(x, axis, n * step)
    return [x] + [copies[n] for n in range(1, length)]


def other_core(x, axis):
    return lax.ppermute(x, axis, [(n, n ^ 1) for n in range(lax.axis_size(axis))])


def whole_step(
    orbital_ints,
    occ_energy,
    pair_row,
    pair_col,
    virt_energy,
    amplitudes,
    intersections,
    coupling_fock,
    partner_owner,
    partner_slot,
):
    rows, cols = lax.axis_size("row"), lax.axis_size("col")
    groups = rows * cols
    size, _, pairs = amplitudes.shape
    cells = size * size
    links = partner_owner.shape[2]
    cap = 2 * pairs * links // groups
    chunk = cap * cells // 128
    per_block = orbital_ints.shape[0]

    make_requests = call(
        functools.partial(request_kernel, cap),
        [jax.ShapeDtypeStruct((groups, 128), F32), jax.ShapeDtypeStruct((links, pairs), I32)],
        [VMEM, VMEM, SMEM],
        flops=10**7,
        nbytes=10**5,
        many=True,
    )
    payload, target = make_requests(partner_owner[0].T, partner_slot[0].T, occ_energy)
    incoming = lax.all_to_all(payload, ("row", "col"), split_axis=0, concat_axis=0, tiled=True)

    gather = call(
        functools.partial(gather_kernel, cap),
        jax.ShapeDtypeStruct((groups, chunk, 128), BF16),
        [VMEM, VMEM],
        scratch=[pltpu.VMEM((groups, cap // 2, pairs), F32)] * 2,
        flops=2 * groups * cap * cells * pairs,
        nbytes=2 * groups * cap * cells,
        grant=14,
    )
    select = call(
        functools.partial(select_kernel, cap),
        jax.ShapeDtypeStruct((links, cells, pairs), BF16),
        [VMEM, VMEM],
        flops=2 * groups * cap * cells * pairs * links,
        nbytes=4 * groups * cap * cells,
        grant=14,
    )

    def returned_tiles(outgoing):
        returned = lax.all_to_all(
            outgoing, ("row", "col"), split_axis=0, concat_axis=0, tiled=True
        )
        return select(target, returned).reshape(links, size, size, pairs)

    def outgoing_tiles(current):
        return gather(incoming, current.reshape(cells, pairs))

    def coupling_of(tiles):
        half_product = jnp.einsum(
            "abcp,cbdp->adcp", intersections, tiles, preferred_element_type=F32
        ).astype(BF16)
        coupled = jnp.einsum(
            "adcp,edcp->aecp", half_product, intersections, preferred_element_type=F32
        )
        return jnp.sum(coupled * coupling_fock[None, None, :, :], axis=2)

    def sum_over_fit(x, y):
        count = lax.axis_size("fit")
        sides = [(n, n ^ 1) for n in range(count)], [(n, count - 1 - n) for n in range(count)]
        part = jax.ShapeDtypeStruct((cells // 2, pairs), BF16)
        halves = call(rounded_kernel, [part] * 2, [VMEM] * 2, nbytes=10**6, many=True)(
            x.reshape(cells, pairs), y.reshape(cells, pairs)
        )
        for turn in range(2):
            there = [lax.ppermute(h, "fit", sides[n ^ turn]) for n, h in enumerate(halves)]
            if turn == 0:
                halves = call(added_kernel, [part] * 2, [VMEM] * 4, nbytes=10**6, many=True)(
                    *halves, *there
                )
        whole = jax.ShapeDtypeStruct((cells, pairs), F32)
        return call(joined_kernel, whole, [VMEM] * 4, nbytes=10**6)(*halves, *there).reshape(
            size, size, pairs
        )

    outgoing, row_blocks, chip_blocks = lax.optimization_barrier(
        (
            outgoing_tiles(amplitudes),
            all_copies(orbital_ints, "col"),
            all_copies(orbital_ints, "row", 2),
        )
    )
    tiles = returned_tiles(outgoing)
    row_ints = stacked(row_blocks)
    core_ints = stacked(chip_blocks)
    col_ints = stacked([core_ints, other_core(core_ints, "row")])
    owner_col, inner_row = pair_row // per_block, pair_row % per_block
    owner_row, inner_col = pair_col // per_block, pair_col % per_block
    my_row, my_col = lax.axis_index("row"), lax.axis_index("col")
    back = (my_col - owner_col) % cols
    chips_back = (my_row // 2 - owner_row // 2) % (rows // 2)
    core_off = (my_row + owner_row) % 2
    kernel = jnp.einsum(
        "pax,pbx->abp",
        row_ints[back * per_block + inner_row],
        col_ints[(core_off * (rows // 2) + chips_back) * per_block + inner_col],
        preferred_element_type=F32,
    )
    energies = incoming[:, cap : cap + per_block].reshape(rows, cols, per_block)
    row_energy = lax.dynamic_index_in_dim(energies, my_row, 0, False).reshape(-1)
    col_energy = lax.dynamic_index_in_dim(energies, my_col, 1, False).reshape(-1)

    def picked(table, index):
        hit = index[None, :] == jnp.arange(table.shape[0], dtype=I32)[:, None]
        return jnp.sum(jnp.where(hit, table[:, None], 0.0), axis=0)

    occupied = picked(row_energy, pair_row) + picked(col_energy, pair_col)
    denominator = virt_energy[:, None, :] + virt_energy[None, :, :] - occupied[None, None, :]

    first = coupling_of(tiles)
    current = sum_over_fit(first, kernel) / denominator
    second = coupling_of(returned_tiles(outgoing_tiles(current)))
    residual = sum_over_fit(first, second)
    return (current - residual / denominator, residual)


def solution(mesh):
    placed = (
        P(("row", "col"), None, "fit"),
        P(("row", "col")),
        P(("row", "col")),
        P(("row", "col")),
        P(None, ("row", "col")),
        P(None, None, ("row", "col")),
        P(None, None, "fit", ("row", "col")),
        P("fit", ("row", "col")),
        P("fit", ("row", "col"), None),
        P("fit", ("row", "col"), None),
    )
    return jax.shard_map(
        whole_step,
        mesh=mesh,
        in_specs=placed,
        out_specs=(P(None, None, ("row", "col")), P(None, None, ("row", "col"))),
        check_vma=False,
    )
```
